32 devices in a mesh: north: 8 (over y, x, core), deep: 4 (over z).
Axes of the slice: x: 2, y: 2, z: 4, core: 2. Of those that a mesh axis runs over, the one named last changes fastest.
Arguments:
- forcing: float32 [2, 128, 128, 256], P(None, None, 'north', 'deep'), may hold values from -6 to 6
- symbol_x: float32 [128], replicated, may hold values from 0.3 to 3
- symbol_y: float32 [128], replicated, may hold values from 0.3 to 3
- symbol_z: float32 [256], replicated, may hold values from 0.3 to 3
Outputs:
- coefficients: float32 [2, 128, 128, 256], P(None, 'north', 'deep')
The draws below stay inside these ranges and needn't reach their ends.
All inputs are finite; a program needn't handle non-finite values.
Results may differ from the reference program's by a relative error of at most 0.000084.
Values sent between devices are 32-bit elements; how exact they have to be, the bound alone decides.
A program may use at most 64 MiB of HBM per device.

```python
import jax
import jax.numpy as jnp
from jax import lax

GRID_X = 128
GRID_Y = 128
GRID_Z = 256
FIELDS = 2


def block_levels(rng, shape, pieces, least, largest):
    level, own = 1.0, jax.random.fold_in(rng, 6)
    for axis_at, blocks in pieces:
        steps = jnp.exp(jax.random.uniform(jax.random.fold_in(own, axis_at), (blocks,), jnp.float32, least / len(pieces), largest / len(pieces)))
        level = level * jnp.repeat(steps, shape[axis_at] // blocks).reshape([-1 if axis == axis_at else 1 for axis in range(len(shape))])
    return level


def bell_draw(rng, shape, spread, bound, cuts=(), dtype=jnp.bfloat16):
    entries = jax.random.normal(rng, shape, jnp.float32) * spread
    if len(cuts) > 0:
        entries = block_levels(rng, shape, cuts, -0.22, 0.18) * entries
    return jnp.clip(entries, min=-bound, max=bound).astype(dtype)


def setup_inputs(seed: int = 0) -> dict:
    splits = jax.random.split(jax.random.key(seed), 5)
    return {
        "forcing": bell_draw(splits[0], (FIELDS, GRID_X, GRID_Y, GRID_Z), 1.0, 6.0, ((2, 8), (3, 4)), jnp.float32),
        "symbol_x": jnp.clip(jax.random.uniform(splits[1], (GRID_X,), jnp.float32, 0.3, 3.0), 0.3, 3.0),
        "symbol_y": jnp.clip(jax.random.uniform(splits[2], (GRID_Y,), jnp.float32, 0.3, 3.0), 0.3, 3.0),
        "symbol_z": jnp.clip(jax.random.uniform(splits[3], (GRID_Z,), jnp.float32, 0.3, 3.0), 0.3, 3.0),
    }


def transform_table(count):
    rank = jnp.arange(count)
    angle = (jnp.pi / (4 * count)) * (((2 * rank[:, None] + 1) * (2 * rank[None, :] + 1)) % (8 * count)).astype(jnp.float32)
    return jnp.cos(angle) * (2.0 / count) ** 0.5


def to_modes(values, dim):
    moved = jnp.tensordot(values, transform_table(values.shape[dim]), axes=([dim], [0]), precision=lax.Precision.HIGHEST)
    return jnp.moveaxis(moved, -1, dim)


def reference(forcing, symbol_x, symbol_y, symbol_z):
    coefficients = forcing
    coefficients = to_modes(coefficients, 1)
    coefficients = to_modes(coefficients, 2)
    coefficients = to_modes(coefficients, 3)
    symbol = symbol_x[:, None, None] + symbol_y[None, :, None] + symbol_z[None, None, :]
    coefficients = coefficients * ((1.0 - 0.2 * symbol) / (1.0 + 0.2 * symbol))
    return coefficients
```

```python
import functools

import jax
import jax.numpy as jnp
import numpy as np
from jax import lax
from jax.experimental import pallas as pl
from jax.experimental.pallas import tpu as pltpu
from jax.sharding import PartitionSpec as P

CHUNKS = 4


def transform_table(count):
    rank = np.arange(count)
    odd = (2 * rank[:, None] + 1) * (2 * rank[None, :] + 1) % (8 * count)
    return (np.cos(np.pi / (4 * count) * odd) * np.sqrt(2.0 / count)).astype(np.float32)


def halves(values):
    high = values.astype(jnp.bfloat16)
    low = (values - high.astype(jnp.float32)).astype(jnp.bfloat16)
    return high, low


def table_halves(table):
    high = table.astype(jnp.bfloat16)
    low = (table - high.astype(np.float32)).astype(jnp.bfloat16)
    return high, low


def partners(me, count):
    found = []
    for step in range(count - 1, 0, -1):
        if count & (count - 1):
            found.append(lax.rem(me + step, count))
            continue
        other = me
        for bit in range(count.bit_length() - 1):
            if step >> bit & 1:
                other = other + (1 - 2 * ((me // 2**bit) % 2)) * 2**bit
        found.append(other)
    return found


def kernel(
    sizes, forcing, hx, hy, hz, sx, sy, sz, out, xin, wa, u, v, r, fac,
    in_sem, ns_sem, nr_sem, ds_sem, dr_sem, own_sem,
):
    north, deep, chunks = sizes
    fields, share_y, share_z, grid_x = forcing.shape
    share_x, part_y = out.shape[1], out.shape[2]
    grid_y, grid_z = v.shape[1], out.shape[3]
    lanes = fields * share_z
    ci = share_x // chunks
    n, d = lax.axis_index("north"), lax.axis_index("deep")
    norths, deeps = partners(n, north), partners(d, deep)

    groups = in_sem.shape[0]
    per = share_y // groups
    loads = []
    for g in range(groups):
        part = (slice(None), pl.ds(g * per, per))
        loads.append(pltpu.make_async_copy(forcing.at[part], xin.at[part], in_sem.at[g]))
        loads[-1].start()
    barrier = pltpu.get_barrier_semaphore()
    for other in norths:
        pl.semaphore_signal(barrier, device_id={"north": other}, device_id_type=pl.DeviceIdType.MESH)
    for other in deeps:
        pl.semaphore_signal(barrier, device_id={"deep": other}, device_id_type=pl.DeviceIdType.MESH)

    pair = 2 if per % 2 == 0 else 1
    for g in range(groups):
        loads[g].wait()
        for y in range(g * per, (g + 1) * per, pair):
            high, low = halves(
                jnp.concatenate([xin[f, y + k] for k in range(pair) for f in range(fields)], axis=0)
            )
            modes = lax.dot_general(
                hx[...],
                jnp.concatenate([high, low, high], axis=1),
                (((1,), (1,)), ((), ())),
                preferred_element_type=jnp.float32,
            )
            for k in range(pair):
                wa[pl.ds(y + k, grid_x, stride=share_y), :] = modes[:, k * lanes : (k + 1) * lanes]

    pl.semaphore_wait(barrier, north + deep - 2)
    block = ci * share_y

    def rows(c, other):
        return pl.ds(pl.multiple_of((c * north + other) * block, block), block)

    def north_copy(c, target, source):
        return pltpu.make_async_remote_copy(
            src_ref=wa.at[rows(c, target)],
            dst_ref=u.at[rows(c, source)],
            send_sem=ns_sem.at[c, target],
            recv_sem=nr_sem.at[c, source],
            device_id={"north": target},
            device_id_type=pl.DeviceIdType.MESH,
        )

    def north_own(c):
        return pltpu.make_async_copy(wa.at[rows(c, n)], u.at[rows(c, n)], own_sem.at[0, c])

    def deep_copy(c, target, source):
        return pltpu.make_async_remote_copy(
            src_ref=v.at[pl.ds(c * ci, ci), pl.ds(pl.multiple_of(target * part_y, part_y), part_y)],
            dst_ref=r.at[source, pl.ds(c * ci, ci)],
            send_sem=ds_sem.at[c, target],
            recv_sem=dr_sem.at[c, source],
            device_id={"deep": target},
            device_id_type=pl.DeviceIdType.MESH,
        )

    def deep_own(c):
        mine = pl.ds(pl.multiple_of(d * part_y, part_y), part_y)
        return pltpu.make_async_copy(
            v.at[pl.ds(c * ci, ci), mine], r.at[d, pl.ds(c * ci, ci)], own_sem.at[1, c]
        )

    for c in range(chunks):
        for other in norths:
            north_copy(c, other, n).start()
        north_own(c).start()

    spot = lax.broadcasted_iota(jnp.int32, (part_y, grid_y), 0) + d * part_y
    along = lax.broadcasted_iota(jnp.int32, (part_y, grid_y), 1)
    column = jnp.sum(jnp.where(spot == along, sy[...], 0.0), axis=1, keepdims=True)
    plane = column + sz[...]
    for i in range(share_x):
        symbol = sx[n * share_x + i] + plane
        fac[pl.ds(i * part_y, part_y), :] = (1.0 - 0.2 * symbol) / (1.0 + 0.2 * symbol)

    pair = 2 if ci % 2 == 0 else 1
    for c in range(chunks):
        for other in norths:
            north_copy(c, n, other).wait_recv()
        north_own(c).wait()
        for i in range(0, ci, pair):
            lines = jnp.concatenate(
                [
                    jnp.concatenate(
                        [
                            u[pl.ds(((c * north + s) * ci + i + k) * share_y, share_y), :]
                            for s in range(north)
                        ],
                        axis=0,
                    )
                    for k in range(pair)
                ],
                axis=1,
            )
            high, low = halves(lines)
            modes = jnp.dot(
                hy[...],
                jnp.concatenate([high, low, high], axis=0),
                preferred_element_type=jnp.float32,
            )
            for k in range(pair):
                v[c * ci + i + k] = modes[:, k * lanes : (k + 1) * lanes]
        for other in deeps:
            deep_copy(c, other, d).start()
        deep_own(c).start()

    for c in range(chunks):
        for other in deeps:
            deep_copy(c, d, other).wait_recv()
        deep_own(c).wait()
        parts = [r[s, pl.ds(c * ci, ci)].reshape(ci * part_y, lanes) for s in range(deep)]
        factor = fac[pl.ds(c * ci * part_y, ci * part_y), :]
        for f in range(fields):
            lines = jnp.concatenate([p[:, f * share_z : (f + 1) * share_z] for p in parts], axis=1)
            high, low = halves(lines)
            modes = jnp.dot(
                jnp.concatenate([high, low, high], axis=1),
                hz[...],
                preferred_element_type=jnp.float32,
            )
            out[f, pl.ds(c * ci, ci)] = (modes * factor).reshape(ci, part_y, grid_z)

    for c in range(chunks):
        for other in norths:
            north_copy(c, other, n).wait_send()
        for other in deeps:
            deep_copy(c, other, d).wait_send()


def local(north, deep, forcing, symbol_x, symbol_y, symbol_z):
    fields, grid_x, share_y, share_z = forcing.shape
    grid_y, grid_z = symbol_y.shape[0], symbol_z.shape[0]
    share_x, part_y = grid_x // north, grid_y // deep
    chunks = CHUNKS if share_x % CHUNKS == 0 else 1
    ci = share_x // chunks
    lanes = fields * share_z

    order = np.arange(grid_x).reshape(north, chunks, ci).transpose(1, 0, 2).reshape(-1)
    high, low = table_halves(transform_table(grid_x)[order])
    hx = np.concatenate([high, high, low], axis=1)
    high, low = table_halves(transform_table(grid_y))
    hy = np.concatenate([high, high, low], axis=1)
    high, low = table_halves(transform_table(grid_z))
    hz = np.concatenate([high, high, low], axis=0)

    groups = 4 if share_y % 4 == 0 else 1
    vmem = pl.BlockSpec(memory_space=pltpu.VMEM)
    return pl.pallas_call(
        functools.partial(kernel, (north, deep, chunks)),
        out_shape=jax.ShapeDtypeStruct((fields, share_x, part_y, grid_z), jnp.float32),
        in_specs=[
            pl.BlockSpec(memory_space=pl.ANY),
            vmem,
            vmem,
            vmem,
            pl.BlockSpec(memory_space=pltpu.SMEM),
            vmem,
            vmem,
        ],
        out_specs=vmem,
        scratch_shapes=[
            pltpu.VMEM((fields, share_y, share_z, grid_x), jnp.float32),
            pltpu.VMEM((grid_x * share_y, lanes), jnp.float32),
            pltpu.VMEM((grid_y * share_x, lanes), jnp.float32),
            pltpu.VMEM((share_x, grid_y, lanes), jnp.float32),
            pltpu.VMEM((deep, share_x, part_y, lanes), jnp.float32),
            pltpu.VMEM((share_x * part_y, grid_z), jnp.float32),
            pltpu.SemaphoreType.DMA((groups,)),
            pltpu.SemaphoreType.DMA((chunks, north)),
            pltpu.SemaphoreType.DMA((chunks, north)),
            pltpu.SemaphoreType.DMA((chunks, deep)),
            pltpu.SemaphoreType.DMA((chunks, deep)),
            pltpu.SemaphoreType.DMA((2, chunks)),
        ],
        compiler_params=pltpu.CompilerParams(collective_id=0, has_side_effects=True),
    )(
        forcing.transpose(0, 2, 3, 1),
        jnp.asarray(hx),
        jnp.asarray(hy),
        jnp.asarray(hz),
        symbol_x,
        symbol_y[None, :],
        symbol_z[None, :],
    )


def solution(mesh):
    placed = (P(None, None, "north", "deep"), P(), P(), P())
    return jax.shard_map(
        functools.partial(local, mesh.shape["north"], mesh.shape["deep"]),
        mesh=mesh,
        in_specs=placed,
        out_specs=P(None, "north", "deep", None),
        check_vma=False,
    )
```

```python
import functools
import math

import jax
import jax.numpy as jnp
import numpy as np
from jax import lax
from jax.experimental import pallas as pl
from jax.experimental.pallas import tpu as pltpu
from jax.sharding import PartitionSpec as P

CHUNKS = (2, 4, 6, 4)


def transform_table(count):
    rank = np.arange(count)
    odd = (2 * rank[:, None] + 1) * (2 * rank[None, :] + 1) % (8 * count)
    return (np.cos(np.pi / (4 * count) * odd) * np.sqrt(2.0 / count)).astype(np.float32)


def chunk_starts(share):
    unit = max(1, share // sum(CHUNKS))
    found, start = [], 0
    for weight in CHUNKS:
        size = min(unit * weight, share - start)
        if size > 0:
            found.append((start, size))
        start += size
    if start < share:
        found.append((start, share - start))
    return tuple(found)


def halves(values):
    high = values.astype(jnp.bfloat16)
    low = (values - high.astype(jnp.float32)).astype(jnp.bfloat16)
    return high, low


def table_halves(table):
    high = table.astype(jnp.bfloat16)
    low = (table - high.astype(np.float32)).astype(jnp.bfloat16)
    return high, low


def partners(me, count):
    found = []
    for step in range(count - 1, 0, -1):
        if count & (count - 1):
            found.append(lax.rem(me + step, count))
            continue
        other = me
        for bit in range(count.bit_length() - 1):
            if step >> bit & 1:
                other = other + (1 - 2 * ((me // 2**bit) % 2)) * 2**bit
        found.append(other)
    return found


def kernel(
    sizes, forcing, tx, ty, tz, sx, sy, sz, out, xin, hx, hy, hz, wa, u, v, r, fac,
    in_sem, table_sem, ns_sem, nr_sem, ds_sem, dr_sem, own_sem,
):
    north, deep, chunks = sizes
    fields, share_y, share_z, grid_x = forcing.shape
    share_x, part_y = out.shape[1], out.shape[2]
    grid_y, grid_z = v.shape[1], out.shape[3]
    lanes = fields * share_z
    n, d = lax.axis_index("north"), lax.axis_index("deep")
    norths, deeps = partners(n, north), partners(d, deep)

    barrier = pltpu.get_barrier_semaphore()
    for other in norths:
        pl.semaphore_signal(barrier, device_id={"north": other}, device_id_type=pl.DeviceIdType.MESH)
    for other in deeps:
        pl.semaphore_signal(barrier, device_id={"deep": other}, device_id_type=pl.DeviceIdType.MESH)

    tables = [
        pltpu.make_async_copy(source, target, table_sem.at[k])
        for k, (source, target) in enumerate(((tx, hx), (ty, hy), (tz, hz)))
    ]
    tables[0].start()
    groups = in_sem.shape[0]
    per = share_y // groups
    loads = []
    for g in range(groups):
        part = (slice(None), pl.ds(g * per, per))
        loads.append(pltpu.make_async_copy(forcing.at[part], xin.at[part], in_sem.at[g]))
        loads[-1].start()
    tables[1].start()
    tables[2].start()

    pair = 2 if per % 2 == 0 else 1
    tables[0].wait()
    for g in range(groups):
        loads[g].wait()
        for y in range(g * per, (g + 1) * per, pair):
            high, low = halves(
                jnp.concatenate([xin[f, y + k] for k in range(pair) for f in range(fields)], axis=0)
            )
            modes = lax.dot_general(
                hx[...],
                jnp.concatenate([high, low, high], axis=1),
                (((1,), (1,)), ((), ())),
                preferred_element_type=jnp.float32,
            )
            for k in range(pair):
                wa[pl.ds(y + k, grid_x, stride=share_y), :] = modes[:, k * lanes : (k + 1) * lanes]

    pl.semaphore_wait(barrier, north + deep - 2)

    def rows(c, other):
        start, size = chunks[c]
        at = (start * north + other * size) * share_y
        return pl.ds(pl.multiple_of(at, share_y), size * share_y)

    def north_copy(c, target, source):
        return pltpu.make_async_remote_copy(
            src_ref=wa.at[rows(c, target)],
            dst_ref=u.at[rows(c, source)],
            send_sem=ns_sem.at[c, target],
            recv_sem=nr_sem.at[c, source],
            device_id={"north": target},
            device_id_type=pl.DeviceIdType.MESH,
        )

    def north_own(c):
        return pltpu.make_async_copy(wa.at[rows(c, n)], u.at[rows(c, n)], own_sem.at[0, c])

    def deep_copy(c, target, source):
        return pltpu.make_async_remote_copy(
            src_ref=v.at[pl.ds(*chunks[c]), pl.ds(pl.multiple_of(target * part_y, part_y), part_y)],
            dst_ref=r.at[source, pl.ds(*chunks[c])],
            send_sem=ds_sem.at[c, target],
            recv_sem=dr_sem.at[c, source],
            device_id={"deep": target},
            device_id_type=pl.DeviceIdType.MESH,
        )

    def deep_own(c):
        mine = pl.ds(pl.multiple_of(d * part_y, part_y), part_y)
        return pltpu.make_async_copy(
            v.at[pl.ds(*chunks[c]), mine], r.at[d, pl.ds(*chunks[c])], own_sem.at[1, c]
        )

    for c in range(len(chunks)):
        for other in norths:
            north_copy(c, other, n).start()
        north_own(c).start()

    spot = lax.broadcasted_iota(jnp.int32, (part_y, grid_y), 0) + d * part_y
    along = lax.broadcasted_iota(jnp.int32, (part_y, grid_y), 1)
    column = jnp.sum(jnp.where(spot == along, sy[...], 0.0), axis=1, keepdims=True)
    plane = column + sz[...]
    for i in range(share_x):
        symbol = sx[n * share_x + i] + plane
        fac[pl.ds(i * part_y, part_y), :] = (1.0 - 0.2 * symbol) / (1.0 + 0.2 * symbol)

    tables[1].wait()
    for c in range(len(chunks)):
        for other in norths:
            north_copy(c, n, other).wait_recv()
        north_own(c).wait()
        start, size = chunks[c]
        for i in range(0, size, 2):
            pair = min(2, size - i)
            lines = jnp.concatenate(
                [
                    jnp.concatenate(
                        [
                            u[pl.ds((start * north + s * size + i + k) * share_y, share_y), :]
                            for s in range(north)
                        ],
                        axis=0,
                    )
                    for k in range(pair)
                ],
                axis=1,
            )
            high, low = halves(lines)
            modes = jnp.dot(
                hy[...],
                jnp.concatenate([high, low, high], axis=0),
                preferred_element_type=jnp.float32,
            )
            for k in range(pair):
                v[start + i + k] = modes[:, k * lanes : (k + 1) * lanes]
        for other in deeps:
            deep_copy(c, other, d).start()
        deep_own(c).start()

    tables[2].wait()
    for c in range(len(chunks)):
        start, size = chunks[c]
        for other in deeps:
            deep_copy(c, d, other).wait_recv()
        deep_own(c).wait()
        parts = [r[s, pl.ds(*chunks[c])].reshape(size * part_y, lanes) for s in range(deep)]
        factor = fac[pl.ds(start * part_y, size * part_y), :]
        for f in range(fields):
            lines = jnp.concatenate([p[:, f * share_z : (f + 1) * share_z] for p in parts], axis=1)
            high, low = halves(lines)
            modes = jnp.dot(
                jnp.concatenate([high, low, high], axis=1),
                hz[...],
                preferred_element_type=jnp.float32,
            )
            out[f, pl.ds(*chunks[c])] = (modes * factor).reshape(size, part_y, grid_z)

    for c in range(len(chunks)):
        for other in norths:
            north_copy(c, other, n).wait_send()
        for other in deeps:
            deep_copy(c, other, d).wait_send()


def local(north, deep, forcing, symbol_x, symbol_y, symbol_z):
    fields, grid_x, share_y, share_z = forcing.shape
    grid_y, grid_z = symbol_y.shape[0], symbol_z.shape[0]
    share_x, part_y = grid_x // north, grid_y // deep
    chunks = chunk_starts(share_x)
    lanes = fields * share_z

    modes = np.arange(grid_x).reshape(north, share_x)
    order = np.concatenate([modes[:, start : start + size].reshape(-1) for start, size in chunks])
    high, low = table_halves(transform_table(grid_x)[order])
    hx = np.concatenate([high, high, low], axis=1)
    high, low = table_halves(transform_table(grid_y))
    hy = np.concatenate([high, high, low], axis=1)
    high, low = table_halves(transform_table(grid_z))
    hz = np.concatenate([high, high, low], axis=0)

    groups = share_y // 4 if share_y % 4 == 0 else 1
    vmem = pl.BlockSpec(memory_space=pltpu.VMEM)
    buffers = [
        pltpu.VMEM((fields, share_y, share_z, grid_x), jnp.float32),
        pltpu.VMEM(hx.shape, jnp.bfloat16),
        pltpu.VMEM(hy.shape, jnp.bfloat16),
        pltpu.VMEM(hz.shape, jnp.bfloat16),
        pltpu.VMEM((grid_x * share_y, lanes), jnp.float32),
        pltpu.VMEM((grid_y * share_x, lanes), jnp.float32),
        pltpu.VMEM((share_x, grid_y, lanes), jnp.float32),
        pltpu.VMEM((deep, share_x, part_y, lanes), jnp.float32),
        pltpu.VMEM((share_x * part_y, grid_z), jnp.float32),
    ]
    result = fields * share_x * part_y * grid_z
    held = sum(math.prod(b.shape) * jnp.dtype(b.dtype).itemsize for b in buffers)
    return pl.pallas_call(
        functools.partial(kernel, (north, deep, chunks)),
        out_shape=pltpu.VMEM((fields, share_x, part_y, grid_z), jnp.float32),
        in_specs=[
            pl.BlockSpec(memory_space=pltpu.HBM),
            pl.BlockSpec(memory_space=pltpu.HBM),
            pl.BlockSpec(memory_space=pltpu.HBM),
            pl.BlockSpec(memory_space=pltpu.HBM),
            pl.BlockSpec(memory_space=pltpu.SMEM),
            vmem,
            vmem,
        ],
        out_specs=vmem,
        scratch_shapes=[
            *buffers,
            pltpu.SemaphoreType.DMA((groups,)),
            pltpu.SemaphoreType.DMA((3,)),
            pltpu.SemaphoreType.DMA((len(chunks), north)),
            pltpu.SemaphoreType.DMA((len(chunks), north)),
            pltpu.SemaphoreType.DMA((len(chunks), deep)),
            pltpu.SemaphoreType.DMA((len(chunks), deep)),
            pltpu.SemaphoreType.DMA((2, len(chunks))),
        ],
        compiler_params=pltpu.CompilerParams(
            collective_id=0, has_side_effects=True, vmem_limit_bytes=max(held + 2**23, 60 * 2**20 - 4 * result)
        ),
    )(
        forcing.transpose(0, 2, 3, 1),
        jnp.asarray(hx),
        jnp.asarray(hy),
        jnp.asarray(hz),
        symbol_x,
        symbol_y[None, :],
        symbol_z[None, :],
    )


def solution(mesh):
    placed = (P(None, None, "north", "deep"), P(), P(), P())
    return jax.shard_map(
        functools.partial(local, mesh.shape["north"], mesh.shape["deep"]),
        mesh=mesh,
        in_specs=placed,
        out_specs=P(None, "north", "deep", None),
        check_vma=False,
    )
```

```python
import functools
import math

import jax
import jax.numpy as jnp
import numpy as np
from jax import lax
from jax.experimental import pallas as pl
from jax.experimental.pallas import tpu as pltpu
from jax.sharding import PartitionSpec as P

CHUNKS = (2, 4, 6, 4)


def transform_table(count):
    rank = np.arange(count)
    odd = (2 * rank[:, None] + 1) * (2 * rank[None, :] + 1) % (8 * count)
    return (np.cos(np.pi / (4 * count) * odd) * np.sqrt(2.0 / count)).astype(np.float32)


def chunk_starts(share):
    unit = max(1, share // sum(CHUNKS))
    found, start = [], 0
    for weight in CHUNKS:
        size = min(unit * weight, share - start)
        if size > 0:
            found.append((start, size))
        start += size
    if start < share:
        found.append((start, share - start))
    return tuple(found)


def halves(values):
    high = values.astype(jnp.bfloat16)
    low = (values - high.astype(jnp.float32)).astype(jnp.bfloat16)
    return high, low


def table_halves(table):
    high = table.astype(jnp.bfloat16)
    low = (table - high.astype(np.float32)).astype(jnp.bfloat16)
    return high, low


def partners(me, count):
    found = []
    for step in range(count - 1, 0, -1):
        if count & (count - 1):
            found.append(lax.rem(me + step, count))
            continue
        other = me
        for bit in range(count.bit_length() - 1):
            if step >> bit & 1:
                other = other + (1 - 2 * ((me // 2**bit) % 2)) * 2**bit
        found.append(other)
    return found


def kernel(
    sizes, forcing, tx, ty, tz, gx, gy, gz, out, sx, sy, sz, xin, hx, hy, hz, wa, u, v, r, fac,
    in_sem, table_sem, ns_sem, nr_sem, ds_sem, dr_sem, own_sem,
):
    north, deep, chunks = sizes
    fields, share_y, share_z, grid_x = forcing.shape
    share_x, part_y = out.shape[1], out.shape[2]
    grid_y, grid_z = v.shape[1], out.shape[3]
    lanes = fields * share_z
    n, d = lax.axis_index("north"), lax.axis_index("deep")
    norths, deeps = partners(n, north), partners(d, deep)

    barrier = pltpu.get_barrier_semaphore()
    for other in norths:
        pl.semaphore_signal(barrier, device_id={"north": other}, device_id_type=pl.DeviceIdType.MESH)
    for other in deeps:
        pl.semaphore_signal(barrier, device_id={"deep": other}, device_id_type=pl.DeviceIdType.MESH)

    tables = [
        pltpu.make_async_copy(source, target, table_sem.at[k])
        for k, (source, target) in enumerate(((tx, hx), (ty, hy), (tz, hz), (gx, sx), (gy, sy), (gz, sz)))
    ]
    tables[0].start()
    groups = in_sem.shape[0]
    per = share_y // groups
    loads = []
    for g in range(groups):
        part = (slice(None), pl.ds(g * per, per))
        loads.append(pltpu.make_async_copy(forcing.at[part], xin.at[part], in_sem.at[g]))
        loads[-1].start()
    for table in tables[1:]:
        table.start()

    pair = 2 if per % 2 == 0 else 1
    tables[0].wait()
    for g in range(groups):
        loads[g].wait()
        for y in range(g * per, (g + 1) * per, pair):
            high, low = halves(
                jnp.concatenate([xin[f, y + k] for k in range(pair) for f in range(fields)], axis=0)
            )
            modes = lax.dot_general(
                hx[...],
                jnp.concatenate([high, low, high], axis=1),
                (((1,), (1,)), ((), ())),
                preferred_element_type=jnp.float32,
            )
            for k in range(pair):
                wa[pl.ds(y + k, grid_x, stride=share_y), :] = modes[:, k * lanes : (k + 1) * lanes]

    pl.semaphore_wait(barrier, north + deep - 2)

    def rows(c, other):
        start, size = chunks[c]
        at = (start * north + other * size) * share_y
        return pl.ds(pl.multiple_of(at, share_y), size * share_y)

    def north_copy(c, target, source):
        return pltpu.make_async_remote_copy(
            src_ref=wa.at[rows(c, target)],
            dst_ref=u.at[rows(c, source)],
            send_sem=ns_sem.at[c, target],
            recv_sem=nr_sem.at[c, source],
            device_id={"north": target},
            device_id_type=pl.DeviceIdType.MESH,
        )

    def north_own(c):
        return pltpu.make_async_copy(wa.at[rows(c, n)], u.at[rows(c, n)], own_sem.at[0, c])

    def deep_copy(c, target, source):
        return pltpu.make_async_remote_copy(
            src_ref=v.at[pl.ds(*chunks[c]), pl.ds(pl.multiple_of(target * part_y, part_y), part_y)],
            dst_ref=r.at[source, pl.ds(*chunks[c])],
            send_sem=ds_sem.at[c, target],
            recv_sem=dr_sem.at[c, source],
            device_id={"deep": target},
            device_id_type=pl.DeviceIdType.MESH,
        )

    def deep_own(c):
        mine = pl.ds(pl.multiple_of(d * part_y, part_y), part_y)
        return pltpu.make_async_copy(
            v.at[pl.ds(*chunks[c]), mine], r.at[d, pl.ds(*chunks[c])], own_sem.at[1, c]
        )

    for c in range(len(chunks)):
        for other in norths:
            north_copy(c, other, n).start()
        north_own(c).start()

    for table in tables[3:]:
        table.wait()
    spot = lax.broadcasted_iota(jnp.int32, (part_y, grid_y), 0) + d * part_y
    along = lax.broadcasted_iota(jnp.int32, (part_y, grid_y), 1)
    column = jnp.sum(jnp.where(spot == along, sy[...], 0.0), axis=1, keepdims=True)
    plane = column + sz[...]
    spot = lax.broadcasted_iota(jnp.int32, (share_x, sx.shape[1]), 0) + n * share_x
    along = lax.broadcasted_iota(jnp.int32, (share_x, sx.shape[1]), 1)
    column = jnp.sum(jnp.where(spot == along, sx[...], 0.0), axis=1, keepdims=True)
    for i in range(share_x):
        symbol = column[i : i + 1] + plane
        fac[pl.ds(i * part_y, part_y), :] = (1.0 - 0.2 * symbol) / (1.0 + 0.2 * symbol)

    tables[1].wait()
    for c in range(len(chunks)):
        for other in norths:
            north_copy(c, n, other).wait_recv()
        north_own(c).wait()
        start, size = chunks[c]
        for i in range(0, size, 2):
            pair = min(2, size - i)
            lines = jnp.concatenate(
                [
                    jnp.concatenate(
                        [
                            u[pl.ds((start * north + s * size + i + k) * share_y, share_y), :]
                            for s in range(north)
                        ],
                        axis=0,
                    )
                    for k in range(pair)
                ],
                axis=1,
            )
            high, low = halves(lines)
            modes = jnp.dot(
                hy[...],
                jnp.concatenate([high, low, high], axis=0),
                preferred_element_type=jnp.float32,
            )
            for k in range(pair):
                v[start + i + k] = modes[:, k * lanes : (k + 1) * lanes]
        for other in deeps:
            deep_copy(c, other, d).start()
        deep_own(c).start()

    tables[2].wait()
    for c in range(len(chunks)):
        start, size = chunks[c]
        for other in deeps:
            deep_copy(c, d, other).wait_recv()
        deep_own(c).wait()
        parts = [r[s, pl.ds(*chunks[c])].reshape(size * part_y, lanes) for s in range(deep)]
        factor = fac[pl.ds(start * part_y, size * part_y), :]
        for f in range(fields):
            lines = jnp.concatenate([p[:, f * share_z : (f + 1) * share_z] for p in parts], axis=1)
            high, low = halves(lines)
            modes = jnp.dot(
                jnp.concatenate([high, low, high], axis=1),
                hz[...],
                preferred_element_type=jnp.float32,
            )
            out[f, pl.ds(*chunks[c])] = (modes * factor).reshape(size, part_y, grid_z)

    for c in range(len(chunks)):
        for other in norths:
            north_copy(c, other, n).wait_send()
        for other in deeps:
            deep_copy(c, other, d).wait_send()


def local(north, deep, forcing, symbol_x, symbol_y, symbol_z):
    fields, grid_x, share_y, share_z = forcing.shape
    grid_y, grid_z = symbol_y.shape[0], symbol_z.shape[0]
    share_x, part_y = grid_x // north, grid_y // deep
    chunks = chunk_starts(share_x)
    lanes = fields * share_z

    modes = np.arange(grid_x).reshape(north, share_x)
    order = np.concatenate([modes[:, start : start + size].reshape(-1) for start, size in chunks])
    high, low = table_halves(transform_table(grid_x)[order])
    hx = np.concatenate([high, high, low], axis=1)
    high, low = table_halves(transform_table(grid_y))
    hy = np.concatenate([high, high, low], axis=1)
    high, low = table_halves(transform_table(grid_z))
    hz = np.concatenate([high, high, low], axis=0)

    groups = share_y // 4 if share_y % 4 == 0 else 1
    vmem = pl.BlockSpec(memory_space=pltpu.VMEM)
    buffers = [
        pltpu.VMEM((fields, share_y, share_z, grid_x), jnp.float32),
        pltpu.VMEM(hx.shape, jnp.bfloat16),
        pltpu.VMEM(hy.shape, jnp.bfloat16),
        pltpu.VMEM(hz.shape, jnp.bfloat16),
        pltpu.VMEM((grid_x * share_y, lanes), jnp.float32),
        pltpu.VMEM((grid_y * share_x, lanes), jnp.float32),
        pltpu.VMEM((share_x, grid_y, lanes), jnp.float32),
        pltpu.VMEM((deep, share_x, part_y, lanes), jnp.float32),
        pltpu.VMEM((share_x * part_y, grid_z), jnp.float32),
    ]
    result = fields * share_x * part_y * grid_z
    held = sum(math.prod(b.shape) * jnp.dtype(b.dtype).itemsize for b in buffers)
    return pl.pallas_call(
        functools.partial(kernel, (north, deep, chunks)),
        out_shape=pltpu.VMEM((fields, share_x, part_y, grid_z), jnp.float32),
        in_specs=[pl.BlockSpec(memory_space=pltpu.HBM)] * 7,
        out_specs=vmem,
        scratch_shapes=[
            pltpu.VMEM((1, grid_x), jnp.float32),
            pltpu.VMEM((1, grid_y), jnp.float32),
            pltpu.VMEM((1, grid_z), jnp.float32),
            *buffers,
            pltpu.SemaphoreType.DMA((groups,)),
            pltpu.SemaphoreType.DMA((6,)),
            pltpu.SemaphoreType.DMA((len(chunks), north)),
            pltpu.SemaphoreType.DMA((len(chunks), north)),
            pltpu.SemaphoreType.DMA((len(chunks), deep)),
            pltpu.SemaphoreType.DMA((len(chunks), deep)),
            pltpu.SemaphoreType.DMA((2, len(chunks))),
        ],
        compiler_params=pltpu.CompilerParams(
            collective_id=0, has_side_effects=True, vmem_limit_bytes=max(held + 2**23, 60 * 2**20 - 4 * result)
        ),
    )(
        forcing.transpose(0, 2, 3, 1),
        jnp.asarray(hx),
        jnp.asarray(hy),
        jnp.asarray(hz),
        symbol_x[None, :],
        symbol_y[None, :],
        symbol_z[None, :],
    )


def solution(mesh):
    placed = (P(None, None, "north", "deep"), P(), P(), P())
    return jax.shard_map(
        functools.partial(local, mesh.shape["north"], mesh.shape["deep"]),
        mesh=mesh,
        in_specs=placed,
        out_specs=P(None, "north", "deep", None),
        check_vma=False,
    )
```

```python
import functools
import math

import jax
import jax.numpy as jnp
import numpy as np
from jax import lax
from jax.experimental import pallas as pl
from jax.experimental.pallas import tpu as pltpu
from jax.sharding import PartitionSpec as P

CHUNKS = (2, 4, 6, 4)


def transform_table(count):
    rank = np.arange(count)
    odd = (2 * rank[:, None] + 1) * (2 * rank[None, :] + 1) % (8 * count)
    return (np.cos(np.pi / (4 * count) * odd) * np.sqrt(2.0 / count)).astype(np.float32)


def chunk_starts(share):
    unit = max(1, share // sum(CHUNKS))
    found, start = [], 0
    for weight in CHUNKS:
        size = min(unit * weight, share - start)
        if size > 0:
            found.append((start, size))
        start += size
    if start < share:
        found.append((start, share - start))
    return tuple(found)


def halves(values):
    high = values.astype(jnp.bfloat16)
    low = (values - high.astype(jnp.float32)).astype(jnp.bfloat16)
    return high, low


def table_halves(table):
    high = table.astype(jnp.bfloat16)
    low = (table - high.astype(np.float32)).astype(jnp.bfloat16)
    return high, low


def partners(me, count):
    found = []
    for step in range(count - 1, 0, -1):
        if count & (count - 1):
            found.append(lax.rem(me + step, count))
            continue
        other = me
        for bit in range(count.bit_length() - 1):
            if step >> bit & 1:
                other = other + (1 - 2 * ((me // 2**bit) % 2)) * 2**bit
        found.append(other)
    return found


def kernel(
    sizes, forcing, tx, ty, tz, gx, gy, gz, out, sx, sy, sz, xin, hx, hy, hz, wa, u, v, r, fac,
    in_sem, table_sem, ns_sem, nr_sem, ds_sem, dr_sem, own_sem,
):
    north, deep, chunks = sizes
    fields, share_y, share_z, grid_x = forcing.shape
    share_x, part_y = out.shape[1], out.shape[2]
    grid_y, grid_z = v.shape[1], out.shape[3]
    lanes = fields * share_z
    n, d = lax.axis_index("north"), lax.axis_index("deep")
    norths, deeps = partners(n, north), partners(d, deep)
    deeps = deeps[1:] + deeps[:1]

    barrier = pltpu.get_barrier_semaphore()
    for other in norths:
        pl.semaphore_signal(barrier, device_id={"north": other}, device_id_type=pl.DeviceIdType.MESH)
    for other in deeps:
        pl.semaphore_signal(barrier, device_id={"deep": other}, device_id_type=pl.DeviceIdType.MESH)

    tables = [
        pltpu.make_async_copy(source, target, table_sem.at[k])
        for k, (source, target) in enumerate(((tx, hx), (ty, hy), (tz, hz), (gx, sx), (gy, sy), (gz, sz)))
    ]
    tables[0].start()
    groups = in_sem.shape[0]
    per = share_y // groups
    loads = []
    for g in range(groups):
        part = (slice(None), pl.ds(g * per, per))
        loads.append(pltpu.make_async_copy(forcing.at[part], xin.at[part], in_sem.at[g]))
        loads[-1].start()
    for table in tables[1:]:
        table.start()

    pair = 2 if per % 2 == 0 else 1
    tables[0].wait()
    for g in range(groups):
        loads[g].wait()
        for y in range(g * per, (g + 1) * per, pair):
            high, low = halves(
                jnp.concatenate([xin[f, y + k] for k in range(pair) for f in range(fields)], axis=0)
            )
            modes = lax.dot_general(
                hx[...],
                jnp.concatenate([high, low, high], axis=1),
                (((1,), (1,)), ((), ())),
                preferred_element_type=jnp.float32,
            )
            for k in range(pair):
                wa[pl.ds(y + k, grid_x, stride=share_y), :] = modes[:, k * lanes : (k + 1) * lanes]

    pl.semaphore_wait(barrier, north + deep - 2)

    def rows(c, other):
        start, size = chunks[c]
        at = (start * north + other * size) * share_y
        return pl.ds(pl.multiple_of(at, share_y), size * share_y)

    def north_copy(c, target, source):
        return pltpu.make_async_remote_copy(
            src_ref=wa.at[rows(c, target)],
            dst_ref=u.at[rows(c, source)],
            send_sem=ns_sem.at[c, target],
            recv_sem=nr_sem.at[c, source],
            device_id={"north": target},
            device_id_type=pl.DeviceIdType.MESH,
        )

    def north_own(c):
        return pltpu.make_async_copy(wa.at[rows(c, n)], u.at[rows(c, n)], own_sem.at[0, c])

    def deep_copy(c, target, source):
        return pltpu.make_async_remote_copy(
            src_ref=v.at[pl.ds(*chunks[c]), pl.ds(pl.multiple_of(target * part_y, part_y), part_y)],
            dst_ref=r.at[source, pl.ds(*chunks[c])],
            send_sem=ds_sem.at[c, target],
            recv_sem=dr_sem.at[c, source],
            device_id={"deep": target},
            device_id_type=pl.DeviceIdType.MESH,
        )

    def deep_own(c):
        mine = pl.ds(pl.multiple_of(d * part_y, part_y), part_y)
        return pltpu.make_async_copy(
            v.at[pl.ds(*chunks[c]), mine], r.at[d, pl.ds(*chunks[c])], own_sem.at[1, c]
        )

    for c in range(len(chunks)):
        for other in norths:
            north_copy(c, other, n).start()
        north_own(c).start()

    for table in tables[3:]:
        table.wait()
    spot = lax.broadcasted_iota(jnp.int32, (part_y, grid_y), 0) + d * part_y
    along = lax.broadcasted_iota(jnp.int32, (part_y, grid_y), 1)
    column = jnp.sum(jnp.where(spot == along, sy[...], 0.0), axis=1, keepdims=True)
    plane = column + sz[...]
    spot = lax.broadcasted_iota(jnp.int32, (share_x, sx.shape[1]), 0) + n * share_x
    along = lax.broadcasted_iota(jnp.int32, (share_x, sx.shape[1]), 1)
    column = jnp.sum(jnp.where(spot == along, sx[...], 0.0), axis=1, keepdims=True)
    for i in range(share_x):
        symbol = column[i : i + 1] + plane
        fac[pl.ds(i * part_y, part_y), :] = (1.0 - 0.2 * symbol) / (1.0 + 0.2 * symbol)

    tables[1].wait()
    for c in range(len(chunks)):
        for other in norths:
            north_copy(c, n, other).wait_recv()
        north_own(c).wait()
        start, size = chunks[c]
        for i in range(0, size, 2):
            pair = min(2, size - i)
            lines = jnp.concatenate(
                [
                    jnp.concatenate(
                        [
                            u[pl.ds((start * north + s * size + i + k) * share_y, share_y), :]
                            for s in range(north)
                        ],
                        axis=0,
                    )
                    for k in range(pair)
                ],
                axis=1,
            )
            high, low = halves(lines)
            modes = jnp.dot(
                hy[...],
                jnp.concatenate([high, low, high], axis=0),
                preferred_element_type=jnp.float32,
            )
            for k in range(pair):
                v[start + i + k] = modes[:, k * lanes : (k + 1) * lanes]
        for other in deeps:
            deep_copy(c, other, d).start()
        deep_own(c).start()

    tables[2].wait()
    for c in range(len(chunks)):
        start, size = chunks[c]
        for other in deeps:
            deep_copy(c, d, other).wait_recv()
        deep_own(c).wait()
        parts = [r[s, pl.ds(*chunks[c])].reshape(size * part_y, lanes) for s in range(deep)]
        factor = fac[pl.ds(start * part_y, size * part_y), :]
        for f in range(fields):
            lines = jnp.concatenate([p[:, f * share_z : (f + 1) * share_z] for p in parts], axis=1)
            high, low = halves(lines)
            modes = jnp.dot(
                jnp.concatenate([high, low, high], axis=1),
                hz[...],
                preferred_element_type=jnp.float32,
            )
            out[f, pl.ds(*chunks[c])] = (modes * factor).reshape(size, part_y, grid_z)

    for c in range(len(chunks)):
        for other in norths:
            north_copy(c, other, n).wait_send()
        for other in deeps:
            deep_copy(c, other, d).wait_send()


def local(north, deep, forcing, symbol_x, symbol_y, symbol_z):
    fields, grid_x, share_y, share_z = forcing.shape
    grid_y, grid_z = symbol_y.shape[0], symbol_z.shape[0]
    share_x, part_y = grid_x // north, grid_y // deep
    chunks = chunk_starts(share_x)
    lanes = fields * share_z

    modes = np.arange(grid_x).reshape(north, share_x)
    order = np.concatenate([modes[:, start : start + size].reshape(-1) for start, size in chunks])
    high, low = table_halves(transform_table(grid_x)[order])
    hx = np.concatenate([high, high, low], axis=1)
    high, low = table_halves(transform_table(grid_y))
    hy = np.concatenate([high, high, low], axis=1)
    high, low = table_halves(transform_table(grid_z))
    hz = np.concatenate([high, high, low], axis=0)

    groups = share_y // 4 if share_y % 4 == 0 else 1
    vmem = pl.BlockSpec(memory_space=pltpu.VMEM)
    buffers = [
        pltpu.VMEM((fields, share_y, share_z, grid_x), jnp.float32),
        pltpu.VMEM(hx.shape, jnp.bfloat16),
        pltpu.VMEM(hy.shape, jnp.bfloat16),
        pltpu.VMEM(hz.shape, jnp.bfloat16),
        pltpu.VMEM((grid_x * share_y, lanes), jnp.float32),
        pltpu.VMEM((grid_y * share_x, lanes), jnp.float32),
        pltpu.VMEM((share_x, grid_y, lanes), jnp.float32),
        pltpu.VMEM((deep, share_x, part_y, lanes), jnp.float32),
        pltpu.VMEM((share_x * part_y, grid_z), jnp.float32),
    ]
    result = fields * share_x * part_y * grid_z
    held = sum(math.prod(b.shape) * jnp.dtype(b.dtype).itemsize for b in buffers)
    return pl.pallas_call(
        functools.partial(kernel, (north, deep, chunks)),
        out_shape=pltpu.VMEM((fields, share_x, part_y, grid_z), jnp.float32),
        in_specs=[pl.BlockSpec(memory_space=pltpu.HBM)] * 7,
        out_specs=vmem,
        scratch_shapes=[
            pltpu.VMEM((1, grid_x), jnp.float32),
            pltpu.VMEM((1, grid_y), jnp.float32),
            pltpu.VMEM((1, grid_z), jnp.float32),
            *buffers,
            pltpu.SemaphoreType.DMA((groups,)),
            pltpu.SemaphoreType.DMA((6,)),
            pltpu.SemaphoreType.DMA((len(chunks), north)),
            pltpu.SemaphoreType.DMA((len(chunks), north)),
            pltpu.SemaphoreType.DMA((len(chunks), deep)),
            pltpu.SemaphoreType.DMA((len(chunks), deep)),
            pltpu.SemaphoreType.DMA((2, len(chunks))),
        ],
        compiler_params=pltpu.CompilerParams(
            collective_id=0, has_side_effects=True, vmem_limit_bytes=max(held + 2**23, 60 * 2**20 - 4 * result)
        ),
    )(
        forcing.transpose(0, 2, 3, 1),
        jnp.asarray(hx),
        jnp.asarray(hy),
        jnp.asarray(hz),
        symbol_x[None, :],
        symbol_y[None, :],
        symbol_z[None, :],
    )


def solution(mesh):
    placed = (P(None, None, "north", "deep"), P(), P(), P())
    return jax.shard_map(
        functools.partial(local, mesh.shape["north"], mesh.shape["deep"]),
        mesh=mesh,
        in_specs=placed,
        out_specs=P(None, "north", "deep", None),
        check_vma=False,
    )
```
